32 devices in a mesh: rows: 4 (over x, core), cols: 8 (over z, y).
Axes of the slice: x: 2, y: 2, z: 4, core: 2. Of those that a mesh axis runs over, the one named last changes fastest.
Arguments:
- user_factors: float32 [16384, 512], P(('rows', 'cols')), may hold values from -1.2 to 1.2
- item_factors: float32 [4096, 512], P('cols'), may hold values from -1.2 to 1.2
- ratings: bfloat16 [16384, 4, 512], P(('rows', 'cols')), may hold values from -6 to 6
- observed: int32 [16384, 4, 512], P(('rows', 'cols')), may hold values 0 or 1
- item_order: int32 [32, 4, 512], P(('rows', 'cols')), may hold values from 0 to 511, each once within a row
- user_noise: float32 [16384, 4, 512], P(('rows', 'cols')), may hold values from -6 to 6
- item_noise: float32 [4, 4096, 512], P(None, 'cols'), may hold values from -6 to 6
Outputs:
- users_out: float32 [16384, 512], P(('rows', 'cols'))
- items_out: float32 [4096, 512], P('cols')
The draws below stay inside these ranges and needn't reach their ends.
Inputs may be any that keep to these rules, and one draw needn't show every extreme that they name: `item_order`: each row of 512 entries names every item of the block once.
All inputs are finite; a program needn't handle non-finite values. No bound on the sum of `observed` on one device may be relied on, other than what follows from the above.
Results may differ from the reference program's by a relative error of at most 0.0003.
Values sent between devices are 32-bit elements; how exact they have to be, the bound alone decides.
A program may use at most 128 MiB of HBM per device.

```python
import jax
import jax.numpy as jnp
from jax import lax

RANK = 512
UB = 512
IB = 512
KSTEPS = 4
USERS = 16384
ITEMS = 4096
GROUPS = 32
N_ROWS = 4
N_COLS = 8


def plant(values, stream_key, least, largest):
    place = [jax.random.randint(jax.random.fold_in(stream_key, axis), (), 0, length) for axis, length in enumerate(values.shape)]
    main_axis = values.shape.index(max(values.shape))
    next_to = place[:main_axis] + [(place[main_axis] + 1) % values.shape[main_axis]] + place[main_axis + 1:]
    return values.at[tuple(place)].set(least).at[tuple(next_to)].set(largest)


def level_of(key, extent, pieces, low, top_value):
    gain, own = 1.0, jax.random.fold_in(key, 6)
    for dim, shards_of in pieces:
        heights = jnp.exp(jax.random.uniform(jax.random.fold_in(own, dim), (shards_of,), jnp.float32, low / len(pieces), top_value / len(pieces)))
        gain = gain * jnp.repeat(heights, extent[dim] // shards_of).reshape([-1 if axis == dim else 1 for axis in range(len(extent))])
    return gain


def normal_values(key, extent, width, limit, split=(), kind=jnp.bfloat16):
    level = level_of(key, extent, split, -0.22, 0.18) if split else 1.0
    entries = jax.random.normal(key, extent, jnp.float32) * width * level
    return jnp.minimum(jnp.maximum(entries, -limit), limit).astype(kind)


def setup_inputs(seed: int = 0) -> dict:
    seeds = jax.random.split(jax.random.key(seed), 8)
    return {
        "user_factors": normal_values(seeds[0], (USERS, RANK), 0.2, 1.2, ((0, 32),), jnp.float32),
        "item_factors": normal_values(seeds[1], (ITEMS, RANK), 0.2, 1.2, ((0, 8),), jnp.float32),
        "ratings": normal_values(seeds[2], (USERS, KSTEPS, IB), 1.0, 6.0, ((0, 32),)),
        "observed": plant((jax.random.randint(seeds[3], (USERS, KSTEPS, IB), 0, 2) < 1).astype(jnp.int32), jax.random.fold_in(seeds[3], 1), 0, 1),
        "item_order": jax.vmap(lambda own: jax.random.permutation(own, IB))(jax.random.split(seeds[4], GROUPS * KSTEPS)).reshape((GROUPS, KSTEPS, IB)).astype(jnp.int32),
        "user_noise": normal_values(seeds[5], (USERS, KSTEPS, RANK), 1.0, 6.0, ((0, 32),), jnp.float32),
        "item_noise": normal_values(seeds[6], (KSTEPS, ITEMS, RANK), 1.0, 6.0, ((1, 8),), jnp.float32),
    }


highest = lax.Precision.HIGHEST
half_step = 0.005
noise_scale = 0.1


def reference(user_factors, item_factors, ratings, observed, item_order, user_noise, item_noise):
    users = user_factors.reshape(N_ROWS, N_COLS, UB, RANK)
    held = item_factors
    rated = ratings.reshape(N_ROWS, N_COLS, UB, KSTEPS, IB)
    seen = observed.reshape(N_ROWS, N_COLS, UB, KSTEPS, IB)
    orders = item_order.reshape(N_ROWS, N_COLS, KSTEPS, IB)
    noises = user_noise.reshape(N_ROWS, N_COLS, UB, KSTEPS, RANK)
    for section in range(KSTEPS):
        if section > 0:
            held = jnp.roll(held, IB, axis=0)
        blocks = held.reshape(N_COLS, IB, RANK)

        def group(inputs):
            users_row, rated_row, seen_row, order_row = inputs
            picked = jnp.take_along_axis(blocks, order_row[:, :, None].astype(jnp.int32), axis=1)
            predicted = jnp.einsum('cuk,cik->cui', users_row, picked, precision=highest)
            errors = seen_row.astype(jnp.float32) * (rated_row.astype(jnp.float32) - predicted)
            grad_user = jnp.einsum('cui,cik->cuk', errors, picked, precision=highest)
            grad_picked = jnp.einsum('cui,cuk->cik', errors, users_row, precision=highest)
            inverse = jnp.argsort(order_row, axis=-1).astype(jnp.int32)
            grad_item = jnp.take_along_axis(grad_picked, inverse[:, :, None], axis=1)
            return grad_user, grad_item

        grad_user, grad_item = lax.map(group, (users, rated[:, :, :, section, :], seen[:, :, :, section, :], orders[:, :, section, :]))
        users = users + half_step * (grad_user - users) + noise_scale * noises[:, :, :, section, :]
        total = jnp.sum(grad_item, axis=0).reshape(N_COLS * IB, RANK)
        held = held + half_step * (total - held) + noise_scale * item_noise[section]
    return users.reshape(N_ROWS * N_COLS * UB, RANK), held
```

```python
import functools

import jax
import jax.numpy as jnp
from jax import lax
from jax.experimental import pallas as pl
from jax.experimental.pallas import tpu as pltpu
from jax.sharding import PartitionSpec as P

half_step = 0.005
noise_scale = 0.1
MESH = pl.DeviceIdType.MESH
NT = (((1,), (1,)), ((), ()))
TN = (((0,), (0,)), ((), ()))
NN = (((1,), (0,)), ((), ()))


def split(x):
    hi = x.astype(jnp.bfloat16)
    return hi, (x - hi.astype(jnp.float32)).astype(jnp.bfloat16)


def dot1(a, b, dims):
    return lax.dot_general(a, b, dims, preferred_element_type=jnp.float32)


def dot3(a, b, dims):
    return dot1(a[0], b[0], dims) + (dot1(a[0], b[1], dims) + dot1(a[1], b[0], dims))


def kernel(
    R, C, K, NC,
    uf, itf, rt, ob, order, un, inz, uout, iout, dmt,
    U, Uhi, Ulo, GU, H, rv, ov, unv, inv, MT, RT, gsend, gown, grecv, S, stg,
    l_d, l_u, l_h, l_r, l_o, l_n, l_i,
    g_s, g_r, x_s, x_r, c_s, c_r, f_s, f_r,
):
    UB, RANK = uf.shape
    IB = itf.shape[0]
    F = RANK // 2
    CH = IB // NC
    N = K * NC
    G = R // 2
    r = lax.axis_index("rows")
    c = lax.axis_index("cols")
    core = lax.rem(r, 2)
    other = 1 - core
    mg = lax.div(r, 2)
    sib = mg * 2 + other
    nxt = lax.rem(c + 1, C)
    prv = lax.rem(c + C - 1, C)

    def peer(d):
        return lax.rem(mg + d, G) * 2 + core

    def cols(h):
        return pl.ds(pl.multiple_of(h * F, F), F)

    u_in = [pltpu.make_async_copy(uf.at[:, pl.ds(h * F, F)], U.at[h], l_u.at[h]) for h in range(2)]
    h_in = [pltpu.make_async_copy(itf.at[:, pl.ds(h * F, F)], H.at[0, h], l_h.at[h]) for h in range(2)]

    def r_in(s):
        return pltpu.make_async_copy(rt.at[s], rv.at[s], l_r.at[s])

    def o_in(s):
        return pltpu.make_async_copy(ob.at[:, s], ov.at[s], l_o.at[s])

    def n_in(s):
        return pltpu.make_async_copy(un.at[:, s], unv.at[s], l_n.at[s])

    def i_in(s):
        return pltpu.make_async_copy(inz.at[s, :, cols(core)], inv.at[s], l_i.at[s])

    for cp in u_in + h_in:
        cp.start()
    for s in range(K):
        r_in(s).start()
        o_in(s).start()
        i_in(s).start()
        n_in(s).start()

    barrier = pltpu.get_barrier_semaphore()
    pl.semaphore_signal(barrier, inc=1, device_id=(sib, c), device_id_type=MESH)
    for d in range(1, G):
        pl.semaphore_signal(barrier, inc=1, device_id=(peer(d), c), device_id_type=MESH)
    pl.semaphore_signal(barrier, inc=1, device_id=(r, nxt), device_id_type=MESH)
    pl.semaphore_signal(barrier, inc=1, device_id=(r, prv), device_id_type=MESH)

    def rows_of(k):
        return pl.ds(pl.multiple_of(k * CH, CH), CH)

    def g_copy(n):
        return pltpu.make_async_remote_copy(
            src_ref=gsend.at[n], dst_ref=grecv.at[n], send_sem=g_s.at[n], recv_sem=g_r.at[n],
            device_id=(sib, c), device_id_type=MESH)

    def x_copy(n, d):
        return pltpu.make_async_remote_copy(
            src_ref=S.at[n, mg], dst_ref=S.at[n, mg], send_sem=x_s.at[n, d - 1], recv_sem=x_r.at[n, d - 1],
            device_id=(peer(d), c), device_id_type=MESH)

    def c_copy(n):
        dst = H.at[lax.div(n, NC) + 1, core, rows_of(lax.rem(n, NC))]
        return pltpu.make_async_remote_copy(
            src_ref=stg.at[n], dst_ref=dst, send_sem=c_s.at[n], recv_sem=c_r.at[n],
            device_id=(r, nxt), device_id_type=MESH)

    def f_copy(n):
        at = H.at[lax.div(n, NC) + 1, core, rows_of(lax.rem(n, NC))]
        return pltpu.make_async_remote_copy(
            src_ref=at, dst_ref=at, send_sem=f_s.at[n], recv_sem=f_r.at[n],
            device_id=(sib, c), device_id_type=MESH)

    def permute(n):
        s, k = lax.div(n, NC), lax.rem(n, NC)
        items = lax.broadcasted_iota(jnp.int32, (CH, IB), 0) + k * CH
        hot = (items == order[s]).astype(jnp.float32).astype(jnp.bfloat16)
        MT[n] = dot1(hot, ov[s].astype(jnp.float32).astype(jnp.bfloat16), NT).astype(jnp.bfloat16)
        RT[n] = dot1(hot, rv[s], NT).astype(jnp.bfloat16)

    def split_users():
        for h in range(2):
            Uhi[h], Ulo[h] = split(U[h])

    for cp in u_in:
        cp.wait()
    split_users()
    r_in(0).wait()
    o_in(0).wait()
    permute(0)
    for cp in h_in:
        cp.wait()
    pl.semaphore_wait(barrier, G + 2)

    def slot(n, carry):
        s, k = lax.div(n, NC), lax.rem(n, NC)

        @pl.when(n < N)
        def _():
            @pl.when(n >= NC)
            def _():
                f_copy(n - NC).wait_recv()

            hs = [split(H[s, h, rows_of(k)]) for h in range(2)]
            pred = dot3(hs[0], (Uhi[0], Ulo[0]), NT) + dot3(hs[1], (Uhi[1], Ulo[1]), NT)
            err = split(MT[n].astype(jnp.float32) * (RT[n].astype(jnp.float32) - pred))
            gsend[n] = dot3(err, (Uhi[other], Ulo[other]), NN)
            g_copy(n).start()
            gown[...] = dot3(err, (Uhi[core], Ulo[core]), NN)

            for h in range(2):
                part = dot3(err, hs[h], TN)

                @pl.when(k == 0)
                def _():
                    GU[h] = part

                @pl.when(k > 0)
                def _():
                    GU[h] += part

            g_copy(n).wait_recv()
            S[n, mg] = gown[...] + grecv[n]
            for d in range(1, G):
                x_copy(n, d).start()

            @pl.when(k == NC - 1)
            def _():
                n_in(s).wait()
                for h in range(2):
                    u = U[h]
                    U[h] = u + half_step * (GU[h] - u) + noise_scale * unv[s, :, pl.ds(h * F, F)]
                split_users()

            @pl.when(n + 1 < N)
            def _():
                @pl.when(k == NC - 1)
                def _():
                    r_in(s + 1).wait()
                    o_in(s + 1).wait()
                permute(n + 1)

        m = n - 1

        @pl.when((m >= 0) & (m < N))
        def _():
            ms, mk = lax.div(m, NC), lax.rem(m, NC)

            @pl.when(mk == 0)
            def _():
                i_in(ms).wait()

            for d in range(1, G):
                x_copy(m, d).wait_recv()
            total = S[m, 0]
            for q in range(1, G):
                total = total + S[m, q]
            old = H[ms, core, rows_of(mk)]
            new = old + half_step * (total - old) + noise_scale * inv[ms, rows_of(mk)]

            @pl.when(ms < K - 1)
            def _():
                stg[m] = new
                c_copy(m).start()

            @pl.when(ms == K - 1)
            def _():
                H[K, core, rows_of(mk)] = new

        w = n - 2

        @pl.when(w >= 0)
        def _():
            @pl.when(w < N - NC)
            def _():
                c_copy(w).wait_recv()
            f_copy(w).start()

        return carry

    lax.fori_loop(0, N + 2, slot, 0)

    for h in range(2):
        uout[:, pl.ds(h * F, F)] = U[h]

    def drain(n, carry):
        g_copy(n).wait_send()
        for d in range(1, G):
            x_copy(n, d).wait_send()
        f_copy(n).wait_send()

        @pl.when(n < N - NC)
        def _():
            c_copy(n).wait_send()

        @pl.when(n >= N - NC)
        def _():
            f_copy(n).wait_recv()
        return carry

    lax.fori_loop(0, N, drain, 0)
    for i, a in enumerate((MT, RT)):
        cp = pltpu.make_async_copy(a.at[0], dmt.at[i], l_d.at[i])
        cp.start()
        cp.wait()
    for h in range(2):
        iout[:, pl.ds(h * F, F)] = H[K, h]


def solution(mesh):
    R, C = mesh.shape["rows"], mesh.shape["cols"]

    def body(user_factors, item_factors, ratings, observed, item_order, user_noise, item_noise):
        UB, K, IB = ratings.shape
        RANK = user_factors.shape[1]
        NC = 4
        F, CH, N, G = RANK // 2, IB // NC, K * NC, R // 2
        rt = jnp.transpose(ratings, (1, 0, 2))
        ob = observed
        un = user_noise
        order = item_order.reshape(K, 1, IB)
        f32, bf16 = jnp.float32, jnp.bfloat16
        DMA = pltpu.SemaphoreType.DMA
        ANY = pl.BlockSpec(memory_space=pl.ANY)
        return pl.pallas_call(
            functools.partial(kernel, R, C, K, NC),
            out_shape=(jax.ShapeDtypeStruct((UB, RANK), f32), jax.ShapeDtypeStruct((IB, RANK), f32), jax.ShapeDtypeStruct((2, CH, UB), bf16)),
            in_specs=[ANY, ANY, ANY, ANY, pl.BlockSpec(memory_space=pltpu.VMEM), ANY, ANY],
            out_specs=(pl.BlockSpec(memory_space=pltpu.VMEM),) * 2 + (ANY,),
            scratch_shapes=[
                pltpu.VMEM((2, UB, F), f32),
                pltpu.VMEM((2, UB, F), bf16),
                pltpu.VMEM((2, UB, F), bf16),
                pltpu.VMEM((2, UB, F), f32),
                pltpu.VMEM((K + 1, 2, IB, F), f32),
                pltpu.VMEM((K, UB, IB), bf16),
                pltpu.VMEM((K, UB, IB), jnp.int32),
                pltpu.VMEM((K, UB, RANK), f32),
                pltpu.VMEM((K, IB, F), f32),
                pltpu.VMEM((N, CH, UB), bf16),
                pltpu.VMEM((N, CH, UB), bf16),
                pltpu.VMEM((N, CH, F), f32),
                pltpu.VMEM((CH, F), f32),
                pltpu.VMEM((N, CH, F), f32),
                pltpu.VMEM((N, G, CH, F), f32),
                pltpu.VMEM((N, CH, F), f32),
                DMA((2,)), DMA((2,)), DMA((2,)), DMA((K,)), DMA((K,)), DMA((K,)), DMA((K,)),
                DMA((N,)), DMA((N,)), DMA((N, G - 1)), DMA((N, G - 1)),
                DMA((N,)), DMA((N,)), DMA((N,)), DMA((N,)),
            ],
            compiler_params=pltpu.CompilerParams(
                collective_id=0, has_side_effects=True, vmem_limit_bytes=62 * 1024 * 1024
            ),
        )(user_factors, item_factors, rt, ob, order, un, item_noise)[:2]

    return jax.shard_map(
        body,
        mesh=mesh,
        in_specs=(
            P(("rows", "cols"), None),
            P("cols", None),
            P(("rows", "cols"), None, None),
            P(("rows", "cols"), None, None),
            P(("rows", "cols"), None, None),
            P(("rows", "cols"), None, None),
            P(None, "cols", None),
        ),
        out_specs=(P(("rows", "cols"), None), P("cols", None)),
        check_vma=False,
    )
```
